32 devices in a mesh: part: 2 (over x), tpa: 4 (over z), tpb: 4 (over y, core).
Axes of the slice: x: 2, y: 2, z: 4, core: 2. Of those that a mesh axis runs over, the one named last changes fastest.
Arguments:
- x: bfloat16 [16, 2048, 2048], P(('part', 'tpb')), parts along dimension 0
- lengths: int32 [16], P(('part', 'tpb')), parts along dimension 0
- k_buf: bfloat16 [16, 2048, 8, 64], P(('part', 'tpb'), None, 'tpa'), parts along dimension 0
- v_buf: bfloat16 [16, 2048, 8, 64], P(('part', 'tpb'), None, 'tpa'), parts along dimension 0
- w_qkv: bfloat16 [4096, 3072], P('part', ('tpa', 'tpb')), parts along dimension 0
- w_o: bfloat16 [4096, 2048], P(('part', 'tpa', 'tpb')), parts along dimension 0
- w_gate_up: bfloat16 [4096, 16384], P('part', ('tpa', 'tpb')), parts along dimension 0
- w_down: bfloat16 [16384, 2048], P(('part', 'tpa', 'tpb')), parts along dimension 0
- g_attn: bfloat16 [4096], P('part'), parts along dimension 0
- g_mlp: bfloat16 [4096], P('part'), parts along dimension 0
Outputs:
- output 1: bfloat16 [16, 2048, 2048], P(('part', 'tpb')), parts along dimension 0
- output 2: bfloat16 [16, 2048, 8, 64], P(('part', 'tpb'), None, 'tpa'), parts along dimension 0
- output 3: bfloat16 [16, 2048, 8, 64], P(('part', 'tpb'), None, 'tpa'), parts along dimension 0
- output 4: bfloat16 [4096, 2048], P('part', 'tpa'), parts along dimension 0
- output 5: bfloat16 [4096, 512], P('part', 'tpa'), parts along dimension 0
- output 6: bfloat16 [4096, 512], P('part', 'tpa'), parts along dimension 0
- output 7: bfloat16 [4096, 2048], P(('part', 'tpa')), parts along dimension 0
- output 8: bfloat16 [4096, 8192], P('part', 'tpa'), parts along dimension 0
- output 9: bfloat16 [4096, 8192], P('part', 'tpa'), parts along dimension 0
- output 10: bfloat16 [16384, 2048], P(('part', 'tpa')), parts along dimension 0
There are 2 independent parts. The reference program is written for one: setup_inputs(seed, part) draws one part's arguments, and reference() takes and returns one part's arrays. A program takes and returns all parts, laid end to end along the dimension named above; each array names one.
All inputs are finite; a program needn't handle non-finite values.
Results may differ from the reference program's by a relative error of at most 0.0141267.
Values are sent between devices in bfloat16 or wider.
A program may use at most 1 GiB of HBM per device.

```python
import math
import jax
import jax.numpy as jnp
from jax import lax

D = 2048
HEADS = 32
KV_HEADS = 8
HEAD = 64
FF = 8192
BATCH = 8
SEQ = 2048
TRAIN_TP = 16
GROUP = HEADS // KV_HEADS
QKV_COLS = KV_HEADS * (GROUP + 2) * HEAD
FF_BLOCK = FF // TRAIN_TP
ROPE_BASE = 500000.0
ROPE_FACTOR = 8.0
LOW_FREQ = 1.0
HIGH_FREQ = 4.0
ORIG_CONTEXT = 8192.0
NORM_EPS = 1e-5
MASK_VALUE = -1e30


def setup_inputs(seed: int = 0, part: int = 0) -> dict:
    part_key = jax.random.fold_in(jax.random.key(seed), part)
    sub_keys = jax.random.split(part_key, 10)
    x_in = jax.random.normal(sub_keys[0], (BATCH, SEQ, D), jnp.float32)
    drawn_len = jax.random.randint(sub_keys[1], (BATCH,), 1, SEQ + 1)
    lengths = jnp.where(jnp.arange(BATCH) == 0, SEQ, drawn_len).astype(jnp.int32)
    k_buf = jax.random.normal(sub_keys[2], (BATCH, SEQ, KV_HEADS, HEAD), jnp.float32)
    v_buf = jax.random.normal(sub_keys[3], (BATCH, SEQ, KV_HEADS, HEAD), jnp.float32)
    qk_scale = jnp.where(jnp.arange(GROUP + 2) <= GROUP, 1.5, 1.0)[:, None]
    w_qkv = (jax.random.normal(sub_keys[4], (D, KV_HEADS, GROUP + 2, HEAD), jnp.float32) * qk_scale * D ** -0.5).reshape(D, QKV_COLS)
    w_o = jax.random.normal(sub_keys[5], (HEADS * HEAD, D), jnp.float32) * (HEADS * HEAD) ** -0.5
    w_gate_up = jax.random.normal(sub_keys[6], (D, 2 * FF), jnp.float32) * D ** -0.5
    w_down = jax.random.normal(sub_keys[7], (FF, D), jnp.float32) * FF ** -0.5
    g_attn = 1.0 + 0.4 * jax.random.normal(sub_keys[8], (D,), jnp.float32)
    g_mlp = 1.0 + 0.4 * jax.random.normal(sub_keys[9], (D,), jnp.float32)
    return {'x': x_in.astype(jnp.bfloat16), 'lengths': lengths, 'k_buf': k_buf.astype(jnp.bfloat16), 'v_buf': v_buf.astype(jnp.bfloat16), 'w_qkv': w_qkv.astype(jnp.bfloat16), 'w_o': w_o.astype(jnp.bfloat16), 'w_gate_up': w_gate_up.astype(jnp.bfloat16), 'w_down': w_down.astype(jnp.bfloat16), 'g_attn': g_attn.astype(jnp.bfloat16), 'g_mlp': g_mlp.astype(jnp.bfloat16)}


def rms_norm(x_in, gain_vec):
    x_wide = x_in.astype(jnp.float32)
    mean_sq = jnp.mean(x_wide * x_wide, axis=-1, keepdims=True)
    return (x_wide * lax.rsqrt(mean_sq + NORM_EPS) * gain_vec.astype(jnp.float32)).astype(jnp.bfloat16)


def rope_tables():
    exponent = jnp.arange(HEAD // 2, dtype=jnp.float32) * (2.0 / HEAD)
    inv_freq = 1.0 / jnp.power(ROPE_BASE, exponent)
    wavelen = 2.0 * math.pi / inv_freq
    smooth = (ORIG_CONTEXT / wavelen - LOW_FREQ) / (HIGH_FREQ - LOW_FREQ)
    blended = (1.0 - smooth) * inv_freq / ROPE_FACTOR + smooth * inv_freq
    rope_freq = jnp.where(wavelen < ORIG_CONTEXT / HIGH_FREQ, inv_freq, jnp.where(wavelen > ORIG_CONTEXT / LOW_FREQ, inv_freq / ROPE_FACTOR, blended))
    angles = jnp.arange(SEQ, dtype=jnp.float32)[:, None] * rope_freq[None, :]
    return jnp.cos(angles), jnp.sin(angles)


def apply_rope(vec_in, cos_tab, sin_tab):
    half_dim = vec_in.shape[-1] // 2
    first_half = vec_in[..., :half_dim]
    second_half = vec_in[..., half_dim:]
    return jnp.concatenate([first_half * cos_tab - second_half * sin_tab, second_half * cos_tab + first_half * sin_tab], axis=-1)


def reference(x, lengths, k_buf, v_buf, w_qkv, w_o, w_gate_up, w_down, g_attn, g_mlp):
    packed = w_qkv.reshape(D, KV_HEADS, GROUP + 2, HEAD)
    w_q = packed[:, :, :GROUP, :].reshape(D, HEADS * HEAD)
    w_k = packed[:, :, GROUP, :].reshape(D, KV_HEADS * HEAD)
    w_v = packed[:, :, GROUP + 1, :].reshape(D, KV_HEADS * HEAD)
    gu_view = w_gate_up.reshape(D, TRAIN_TP, 2, FF_BLOCK)
    w_gate = gu_view[:, :, 0, :].reshape(D, FF)
    w_up = gu_view[:, :, 1, :].reshape(D, FF)
    cos_tab, sin_tab = rope_tables()
    positions = jnp.arange(SEQ)
    causal = positions[None, :] <= positions[:, None]

    def one_prompt(prompt_item):
        tokens, length = prompt_item
        x_normed = rms_norm(tokens, g_attn)
        queries = jnp.dot(x_normed, w_q, preferred_element_type=jnp.float32).astype(jnp.bfloat16).reshape(SEQ, KV_HEADS, GROUP, HEAD)
        keys_new = jnp.dot(x_normed, w_k, preferred_element_type=jnp.float32).astype(jnp.bfloat16).reshape(SEQ, KV_HEADS, HEAD)
        values = jnp.dot(x_normed, w_v, preferred_element_type=jnp.float32).astype(jnp.bfloat16).reshape(SEQ, KV_HEADS, HEAD)
        q_rot = apply_rope(queries.astype(jnp.float32), cos_tab[:, None, None, :], sin_tab[:, None, None, :]).astype(jnp.bfloat16)
        k_rot = apply_rope(keys_new.astype(jnp.float32), cos_tab[:, None, :], sin_tab[:, None, :]).astype(jnp.bfloat16)
        allowed = causal & (positions[None, :] < length)

        def one_group(kv_item):
            q_head, k_head, v_head = kv_item
            scores = jnp.einsum('qgd,sd->gqs', q_head.astype(jnp.float32), k_head.astype(jnp.float32)) * HEAD ** -0.5
            scores = jnp.where(allowed[None], scores, MASK_VALUE)
            attn_prob = jax.nn.softmax(scores, axis=-1).astype(jnp.bfloat16)
            return jnp.einsum('gqs,sd->qgd', attn_prob.astype(jnp.float32), v_head.astype(jnp.float32)).astype(jnp.bfloat16)

        per_group = lax.map(one_group, (q_rot.transpose(1, 0, 2, 3), k_rot.transpose(1, 0, 2), values.transpose(1, 0, 2)))
        attn_out = per_group.transpose(1, 0, 2, 3).reshape(SEQ, HEADS * HEAD)
        attn_proj = jnp.dot(attn_out, w_o, preferred_element_type=jnp.float32)
        hidden = (tokens.astype(jnp.float32) + attn_proj).astype(jnp.bfloat16)
        h_normed = rms_norm(hidden, g_mlp)
        gate_act = jnp.dot(h_normed, w_gate, preferred_element_type=jnp.float32).astype(jnp.bfloat16)
        up_act = jnp.dot(h_normed, w_up, preferred_element_type=jnp.float32).astype(jnp.bfloat16)
        mid_act = (jax.nn.silu(gate_act.astype(jnp.float32)) * up_act.astype(jnp.float32)).astype(jnp.bfloat16)
        layer_out = (hidden.astype(jnp.float32) + jnp.dot(mid_act, w_down, preferred_element_type=jnp.float32)).astype(jnp.bfloat16)
        return layer_out, k_rot, values

    layer_out, k_new, v_new = lax.map(one_prompt, (x, lengths))
    valid_pos = (positions[None, :] < lengths[:, None])[:, :, None, None]
    k_cache = jnp.where(valid_pos, k_new, k_buf)
    v_cache = jnp.where(valid_pos, v_new, v_buf)
    return (layer_out, k_cache, v_cache, w_q, w_k, w_v, w_o, w_gate, w_up, w_down)
```

```python
import functools
import math
import jax
import jax.numpy as jnp
from jax import lax
from jax.sharding import PartitionSpec as P
from jax.experimental import pallas as pl
from jax.experimental.pallas import tpu as pltpu

ROPE_BASE = 500000.0
ROPE_FACTOR = 8.0
LOW_FREQ = 1.0
HIGH_FREQ = 4.0
ORIG_CONTEXT = 8192.0
NORM_EPS = 1e-5
MASK_VALUE = -1e30
HEAD = 64
LANES = 128

FAR_ROW = [(0, 2), (2, 0), (1, 3), (3, 1)]
NEAR_ROW = [(0, 1), (1, 0), (2, 3), (3, 2)]
OTHER_CHIP = [(0, 2), (2, 0), (1, 3), (3, 1)]
OTHER_CORE = [(0, 1), (1, 0), (2, 3), (3, 2)]
INWARD = [(0, 1), (3, 2)]
ACROSS = [(1, 2), (2, 1)]
OUTWARD = [(1, 0), (2, 3)]


def rms_norm(x_in, gain_vec):
    x_wide = x_in.astype(jnp.float32)
    mean_sq = jnp.mean(x_wide * x_wide, axis=-1, keepdims=True)
    return (x_wide * lax.rsqrt(mean_sq + NORM_EPS) * gain_vec.astype(jnp.float32)).astype(jnp.bfloat16)


def rope_tables(seq_len, head_dim):
    exponent = jnp.arange(head_dim // 2, dtype=jnp.float32) * (2.0 / head_dim)
    inv_freq = 1.0 / jnp.power(ROPE_BASE, exponent)
    wavelen = 2.0 * math.pi / inv_freq
    smooth = (ORIG_CONTEXT / wavelen - LOW_FREQ) / (HIGH_FREQ - LOW_FREQ)
    blended = (1.0 - smooth) * inv_freq / ROPE_FACTOR + smooth * inv_freq
    rope_freq = jnp.where(wavelen < ORIG_CONTEXT / HIGH_FREQ, inv_freq, jnp.where(wavelen > ORIG_CONTEXT / LOW_FREQ, inv_freq / ROPE_FACTOR, blended))
    angles = jnp.arange(seq_len, dtype=jnp.float32)[:, None] * rope_freq[None, :]
    return jnp.cos(angles), jnp.sin(angles)


def apply_rope(vec_in, cos_tab, sin_tab):
    half_dim = vec_in.shape[-1] // 2
    first_half = vec_in[..., :half_dim]
    second_half = vec_in[..., half_dim:]
    return jnp.concatenate([first_half * cos_tab - second_half * sin_tab, second_half * cos_tab + first_half * sin_tab], axis=-1)


def attn_kernel(tile, q_ref, kv_ref, cos_ref, sin_ref, aug_ref, o_ref, qe_s, qo_s, k_s, ve_s, vo_s):
    seq = q_ref.shape[0]
    lane = lax.broadcasted_iota(jnp.int32, (tile, LANES), 1)
    low = lane < HEAD
    first = lax.rem(lane, HEAD) < HEAD // 2
    ones = jnp.ones((tile, LANES), jnp.float32)
    hot = jnp.where(lane == HEAD, 1.0, 0.0)

    def rope(val, cos, sin):
        rot = jnp.where(first, pltpu.roll(val, LANES - HEAD // 2, 1), pltpu.roll(val, HEAD // 2, 1))
        return val * cos + rot * sin

    for i in range(seq // tile):
        rows = slice(i * tile, (i + 1) * tile)
        cos, sin = cos_ref[rows, :], sin_ref[rows, :]
        q = rope(q_ref[rows, :].astype(jnp.float32), cos, sin).astype(jnp.bfloat16).astype(jnp.float32) * HEAD ** -0.5
        qe_s[rows, :] = jnp.where(low, q, hot).astype(jnp.bfloat16)
        qo_s[rows, :] = jnp.where(low, pltpu.roll(q, HEAD, 1), hot).astype(jnp.bfloat16)
        kv = kv_ref[rows, :].astype(jnp.float32)
        k_s[rows, :] = jnp.where(low, rope(kv, cos, sin), aug_ref[rows, :].astype(jnp.float32)).astype(jnp.bfloat16)
        ve_s[rows, :] = jnp.where(low, pltpu.roll(kv, HEAD, 1), ones).astype(jnp.bfloat16)
        vo_s[rows, :] = jnp.where(low, ones, kv).astype(jnp.bfloat16)
    causal = lax.broadcasted_iota(jnp.int32, (tile, tile), 1) <= lax.broadcasted_iota(jnp.int32, (tile, tile), 0)
    dims = (((1,), (1,)), ((), ()))
    for i in range(seq // tile):
        rows = slice(i * tile, (i + 1) * tile)
        outs = []
        for qs, vs in ((qe_s, ve_s), (qo_s, vo_s)):
            q = qs[rows, :]
            diag = jnp.where(causal, lax.dot_general(q, k_s[rows, :], dims, preferred_element_type=jnp.float32), MASK_VALUE)
            top = jnp.max(diag, axis=1, keepdims=True)
            if i:
                past = lax.dot_general(q, k_s[:i * tile, :], dims, preferred_element_type=jnp.float32)
                top = jnp.maximum(top, jnp.max(past, axis=1, keepdims=True))
            out = jnp.dot(jnp.exp(diag - top).astype(jnp.bfloat16), vs[rows, :], preferred_element_type=jnp.float32)
            if i:
                out = out + jnp.dot(jnp.exp(past - top).astype(jnp.bfloat16), vs[:i * tile, :], preferred_element_type=jnp.float32)
            outs.append(out)
        num = jnp.where(low, outs[0], outs[1])
        den = pltpu.roll(jnp.where(low, outs[1], outs[0]), HEAD, 1)
        o_ref[rows, :] = (num / den).astype(jnp.bfloat16)


def attention(qkv, cos, sin, aug):
    seq, cols = qkv.shape
    groups = cols // (3 * LANES)
    tile = min(512, seq)

    def block(index):
        return pl.BlockSpec((seq, LANES), index)

    return pl.pallas_call(
        functools.partial(attn_kernel, tile),
        grid=(groups, 2),
        in_specs=[block(lambda g, p: (0, 3 * g + p)), block(lambda g, p: (0, 3 * g + 2)), block(lambda g, p: (0, 0)), block(lambda g, p: (0, 0)), block(lambda g, p: (0, 0))],
        out_specs=block(lambda g, p: (0, 2 * g + p)),
        out_shape=jax.ShapeDtypeStruct((seq, groups * 2 * LANES), jnp.bfloat16),
        scratch_shapes=[pltpu.VMEM((seq, LANES), jnp.bfloat16)] * 5,
        cost_estimate=pl.CostEstimate(flops=groups * 16 * seq * seq * LANES, bytes_accessed=seq * groups * 2560, transcendentals=groups * 2 * seq * seq),
        name="attention",
    )(qkv, qkv, cos, sin, aug)


def place_kernel(base_ref, *refs):
    for k in range(4):
        @pl.when(pl.program_id(0) == k)
        def _(k=k):
            refs[4][...] = refs[k][...]


def place(srcs, base, width, col, by_rows):
    rows = srcs[0].shape[0]
    tile = min(256, rows)
    steps = rows // tile

    def source(k):
        return pl.BlockSpec((tile, width), lambda r, i, base: (jnp.where(r == k, i, jnp.where(r < k, 0, steps - 1)), col))

    def target(r, i, base):
        spot = base[0] ^ r
        return (spot * steps + i, 0) if by_rows else (i, spot)

    shape = (4 * rows, width) if by_rows else (rows, 4 * width)
    return pl.pallas_call(
        place_kernel,
        grid_spec=pltpu.PrefetchScalarGridSpec(num_scalar_prefetch=1, grid=(4, steps), in_specs=[source(k) for k in range(4)], out_specs=pl.BlockSpec((tile, width), target)),
        out_shape=jax.ShapeDtypeStruct(shape, srcs[0].dtype),
        cost_estimate=pl.CostEstimate(flops=4 * rows * width * 512, bytes_accessed=16 * rows * width, transcendentals=0),
        name="place",
    )(base.reshape(1).astype(jnp.int32), *srcs)


def gather_blocks(block):
    chip = lax.ppermute(block, 'tpb', OTHER_CHIP)
    core = lax.ppermute(block, 'tpb', OTHER_CORE)
    return block, core, chip, lax.ppermute(chip, 'tpb', OTHER_CORE)


def dot(a, b):
    return jnp.dot(a, b, preferred_element_type=jnp.float32)


def local_step(x_loc, len_loc, k_buf, v_buf, w_qkv, w_o, w_gate_up, w_down, g_attn, g_mlp):
    batch, seq, model_dim = x_loc.shape
    tpa = lax.axis_index('tpa')
    tpb = lax.axis_index('tpb')
    ff_block = w_down.shape[0]
    x_flat = x_loc.reshape(batch * seq, model_dim)

    qkv_own = lax.all_gather(w_qkv, 'tpb', axis=1, tiled=True)
    far = lax.ppermute(w_qkv, 'tpa', FAR_ROW)
    qkv_far = lax.all_gather(far, 'tpb', axis=1, tiled=True)
    w_o_all = lax.all_gather(w_o, ('tpa', 'tpb'), axis=0, tiled=True)
    w_gate_up, w_down, _ = lax.optimization_barrier((w_gate_up, w_down, qkv_own))
    gu = gather_blocks(w_gate_up)
    down = gather_blocks(w_down)
    w_gate = place(gu, tpb, ff_block, 0, False)
    w_up = place(gu, tpb, ff_block, 1, False)
    w_down_gen = place(down, tpb, model_dim, 0, True)

    cos_tab, sin_tab = rope_tables(seq, HEAD)
    cos_wide = jnp.tile(cos_tab, (1, 4))
    sin_wide = jnp.tile(jnp.concatenate([-sin_tab, sin_tab], axis=1), (1, 2))
    positions = jnp.arange(seq)
    at_mask = (jnp.arange(LANES) == HEAD)[None, None, :] & (positions[None, :, None] >= len_loc[:, None, None])
    aug = jnp.where(at_mask, MASK_VALUE, 0.0).astype(jnp.bfloat16)

    normed = rms_norm(x_flat, g_attn)
    act_own = dot(normed, qkv_own).astype(jnp.bfloat16).reshape(batch, seq, -1)
    act_far = dot(normed, qkv_far).astype(jnp.bfloat16).reshape(batch, seq, -1)
    heads_own = [attention(act_own[b], cos_wide, sin_wide, aug[b]) for b in range(batch)]
    near_own = [lax.ppermute(h, 'tpa', NEAR_ROW) for h in heads_own]
    heads_far = [attention(act_far[b], cos_wide, sin_wide, aug[b]) for b in range(batch)]
    near_far = [lax.ppermute(h, 'tpa', NEAR_ROW) for h in heads_far]

    is_middle = (tpa == 1) | (tpa == 2)
    sixteenth = seq // 8
    plans = [(1, 1, 2, 2, 2), (2, 2, 2, 1, 1)]
    chunks = []
    for b in range(batch):
        attn_out = place((heads_own[b], near_own[b], heads_far[b], near_far[b]), tpa, heads_own[b].shape[1], 0, False)
        hidden = (x_loc[b].astype(jnp.float32) + dot(attn_out, w_o_all)).astype(jnp.bfloat16)
        mlp_in = rms_norm(hidden, g_mlp)
        start = 0
        for step in plans[min(b, 1)]:
            rows = slice(start, start + step * sixteenth)
            chunks.append((b, start, hidden[rows], mlp_in[rows]))
            start += step * sixteenth

    layer_out = jnp.zeros((batch, seq, model_dim), jnp.bfloat16)
    count = len(chunks)
    parts, inward, halves, across, outs, outward = {}, {}, {}, {}, {}, {}
    held = ()
    for k in range(count + 3):
        if k < count:
            tied = lax.optimization_barrier((chunks[k][3], layer_out) + held)
            normed_rows, layer_out = tied[:2]
            gate = dot(normed_rows, w_gate).astype(jnp.bfloat16)
            up = dot(normed_rows, w_up).astype(jnp.bfloat16)
            mid = (jax.nn.silu(gate.astype(jnp.float32)) * up.astype(jnp.float32)).astype(jnp.bfloat16)
            parts[k] = dot(mid, w_down_gen).astype(jnp.bfloat16)
            inward[k] = lax.ppermute(parts[k], 'tpa', INWARD)
        held = ()
        j = k - 1
        if 0 <= j < count:
            halves[j] = lax.optimization_barrier((parts[j].astype(jnp.float32) + inward[j].astype(jnp.float32)).astype(jnp.bfloat16))
            across[j] = lax.ppermute(halves[j], 'tpa', ACROSS)
            held += (halves[j],)
        j = k - 2
        if 0 <= j < count:
            total = halves[j].astype(jnp.float32) + across[j].astype(jnp.float32)
            outs[j] = lax.optimization_barrier((chunks[j][2].astype(jnp.float32) + total).astype(jnp.bfloat16))
            outward[j] = lax.ppermute(outs[j], 'tpa', OUTWARD)
            held += (outs[j],)
        j = k - 3
        if 0 <= j < count:
            done = jnp.where(is_middle, outs[j], outward[j])
            layer_out = lax.dynamic_update_slice(layer_out, done[None], (chunks[j][0], chunks[j][1], 0))

    kv_local = k_buf.shape[2]
    width = act_own.shape[2] // kv_local
    q_width = width - 2 * HEAD

    def columns(array, begin, size):
        return [array[..., g * width + begin:g * width + begin + size] for g in range(kv_local)]

    k_new = jnp.stack(columns(act_own, q_width, HEAD), axis=2)
    values = jnp.stack(columns(act_own, q_width + HEAD, HEAD), axis=2)
    k_rot = apply_rope(k_new.astype(jnp.float32), cos_tab[:, None, :], sin_tab[:, None, :]).astype(jnp.bfloat16)
    valid = (positions[None, :] < len_loc[:, None])[:, :, None, None]
    k_cache = jnp.where(valid, k_rot, k_buf)
    v_cache = jnp.where(valid, values, v_buf)

    w_query = jnp.concatenate(columns(qkv_own, 0, q_width), axis=1)
    w_key = jnp.concatenate(columns(qkv_own, q_width, HEAD), axis=1)
    w_value = jnp.concatenate(columns(qkv_own, q_width + HEAD, HEAD), axis=1)
    o_rows = w_o_all.shape[0] // 4
    w_o_gen = lax.dynamic_slice(w_o_all, (tpa * o_rows, 0), (o_rows, w_o_all.shape[1]))
    return (layer_out, k_cache, v_cache, w_query, w_key, w_value, w_o_gen, w_gate, w_up, w_down_gen)


def solution(mesh):
    batch_spec = P(('part', 'tpb'), None, None)
    len_spec = P(('part', 'tpb'))
    cache_spec = P(('part', 'tpb'), None, 'tpa', None)
    train_cols = P('part', ('tpa', 'tpb'))
    train_rows = P(('part', 'tpa', 'tpb'), None)
    gain_spec = P('part')
    gen_cols = P('part', 'tpa')
    gen_rows = P(('part', 'tpa'), None)
    return jax.shard_map(local_step, mesh=mesh, in_specs=(batch_spec, len_spec, cache_spec, cache_spec, train_cols, train_rows, train_cols, train_rows, gain_spec, gain_spec), out_specs=(batch_spec, cache_spec, cache_spec, gen_cols, gen_cols, gen_cols, gen_rows, gen_cols, gen_cols, gen_rows), check_vma=False)
```

```python
import functools
import math
import jax
import jax.numpy as jnp
from jax import lax
from jax.sharding import PartitionSpec as P
from jax.experimental import pallas as pl
from jax.experimental.pallas import tpu as pltpu

ROPE_BASE = 500000.0
ROPE_FACTOR = 8.0
LOW_FREQ = 1.0
HIGH_FREQ = 4.0
ORIG_CONTEXT = 8192.0
NORM_EPS = 1e-5
MASK_VALUE = -1e30
HEAD = 64
LANES = 128

FAR_ROW = [(0, 2), (2, 0), (1, 3), (3, 1)]
NEAR_ROW = [(0, 1), (1, 0), (2, 3), (3, 2)]
OTHER_CHIP = [(0, 2), (2, 0), (1, 3), (3, 1)]
OTHER_CORE = [(0, 1), (1, 0), (2, 3), (3, 2)]


def rms_norm(x_in, gain_vec):
    x_wide = x_in.astype(jnp.float32)
    mean_sq = jnp.mean(x_wide * x_wide, axis=-1, keepdims=True)
    return (x_wide * lax.rsqrt(mean_sq + NORM_EPS) * gain_vec.astype(jnp.float32)).astype(jnp.bfloat16)


def rope_tables(seq_len, head_dim):
    exponent = jnp.arange(head_dim // 2, dtype=jnp.float32) * (2.0 / head_dim)
    inv_freq = 1.0 / jnp.power(ROPE_BASE, exponent)
    wavelen = 2.0 * math.pi / inv_freq
    smooth = (ORIG_CONTEXT / wavelen - LOW_FREQ) / (HIGH_FREQ - LOW_FREQ)
    blended = (1.0 - smooth) * inv_freq / ROPE_FACTOR + smooth * inv_freq
    rope_freq = jnp.where(wavelen < ORIG_CONTEXT / HIGH_FREQ, inv_freq, jnp.where(wavelen > ORIG_CONTEXT / LOW_FREQ, inv_freq / ROPE_FACTOR, blended))
    angles = jnp.arange(seq_len, dtype=jnp.float32)[:, None] * rope_freq[None, :]
    return jnp.cos(angles), jnp.sin(angles)


def apply_rope(vec_in, cos_tab, sin_tab):
    half_dim = vec_in.shape[-1] // 2
    first_half = vec_in[..., :half_dim]
    second_half = vec_in[..., half_dim:]
    return jnp.concatenate([first_half * cos_tab - second_half * sin_tab, second_half * cos_tab + first_half * sin_tab], axis=-1)


def attn_kernel(tile, q_ref, kv_ref, cos_ref, sin_ref, aug_ref, o_ref, qe_s, qo_s, k_s, ve_s, vo_s):
    seq = q_ref.shape[0]
    lane = lax.broadcasted_iota(jnp.int32, (tile, LANES), 1)
    low = lane < HEAD
    first = lax.rem(lane, HEAD) < HEAD // 2
    ones = jnp.ones((tile, LANES), jnp.float32)
    hot = jnp.where(lane == HEAD, 1.0, 0.0)

    def rope(val, cos, sin):
        rot = jnp.where(first, pltpu.roll(val, LANES - HEAD // 2, 1), pltpu.roll(val, HEAD // 2, 1))
        return val * cos + rot * sin

    for i in range(seq // tile):
        rows = slice(i * tile, (i + 1) * tile)
        cos, sin = cos_ref[rows, :], sin_ref[rows, :]
        q = rope(q_ref[rows, :].astype(jnp.float32), cos, sin).astype(jnp.bfloat16).astype(jnp.float32) * HEAD ** -0.5
        qe_s[rows, :] = jnp.where(low, q, hot).astype(jnp.bfloat16)
        qo_s[rows, :] = jnp.where(low, pltpu.roll(q, HEAD, 1), hot).astype(jnp.bfloat16)
        kv = kv_ref[rows, :].astype(jnp.float32)
        k_s[rows, :] = jnp.where(low, rope(kv, cos, sin), aug_ref[rows, :].astype(jnp.float32)).astype(jnp.bfloat16)
        ve_s[rows, :] = jnp.where(low, pltpu.roll(kv, HEAD, 1), ones).astype(jnp.bfloat16)
        vo_s[rows, :] = jnp.where(low, ones, kv).astype(jnp.bfloat16)
    causal = lax.broadcasted_iota(jnp.int32, (tile, tile), 1) <= lax.broadcasted_iota(jnp.int32, (tile, tile), 0)
    dims = (((1,), (1,)), ((), ()))
    for i in range(seq // tile):
        rows = slice(i * tile, (i + 1) * tile)
        outs = []
        for qs, vs in ((qe_s, ve_s), (qo_s, vo_s)):
            q = qs[rows, :]
            diag = jnp.where(causal, lax.dot_general(q, k_s[rows, :], dims, preferred_element_type=jnp.float32), MASK_VALUE)
            top = jnp.max(diag, axis=1, keepdims=True)
            if i:
                past = lax.dot_general(q, k_s[:i * tile, :], dims, preferred_element_type=jnp.float32)
                top = jnp.maximum(top, jnp.max(past, axis=1, keepdims=True))
            out = jnp.dot(jnp.exp(diag - top).astype(jnp.bfloat16), vs[rows, :], preferred_element_type=jnp.float32)
            if i:
                out = out + jnp.dot(jnp.exp(past - top).astype(jnp.bfloat16), vs[:i * tile, :], preferred_element_type=jnp.float32)
            outs.append(out)
        num = jnp.where(low, outs[0], outs[1])
        den = pltpu.roll(jnp.where(low, outs[1], outs[0]), HEAD, 1)
        o_ref[rows, :] = (num / den).astype(jnp.bfloat16)


def attention(qkv, cos, sin, aug, batch):
    rows, cols = qkv.shape
    seq = rows // batch
    groups = cols // (3 * LANES)
    tile = min(512, seq)

    def block(index):
        return pl.BlockSpec((seq, LANES), index)

    return pl.pallas_call(
        functools.partial(attn_kernel, tile),
        grid=(batch, groups, 2),
        in_specs=[block(lambda b, g, p: (b, 3 * g + p)), block(lambda b, g, p: (b, 3 * g + 2)), block(lambda b, g, p: (0, 0)), block(lambda b, g, p: (0, 0)), block(lambda b, g, p: (b, 0))],
        out_specs=block(lambda b, g, p: (b, 2 * g + p)),
        out_shape=jax.ShapeDtypeStruct((rows, groups * 2 * LANES), jnp.bfloat16),
        scratch_shapes=[pltpu.VMEM((seq, LANES), jnp.bfloat16)] * 5,
        cost_estimate=pl.CostEstimate(flops=groups * batch * 16 * seq * seq * LANES, bytes_accessed=rows * groups * 2560, transcendentals=batch * groups * 2 * seq * seq),
        name="attention",
    )(qkv, qkv, cos, sin, aug)


def place_kernel(base_ref, *refs):
    outs = refs[4:]
    width = outs[0].shape[1]
    for k in range(4):
        @pl.when(pl.program_id(0) == k)
        def _(k=k):
            for n, out in enumerate(outs):
                out[...] = refs[k][:, n * width:(n + 1) * width]


def place(srcs, base, count, by_rows):
    rows, cols = srcs[0].shape
    width = cols // count
    tile = min(512, rows)
    steps = rows // tile

    def source(k):
        return pl.BlockSpec((tile, cols), lambda r, i, base: (jnp.where(r == k, i, jnp.where(r < k, 0, steps - 1)), 0))

    def target(r, i, base):
        spot = base[0] ^ r
        return (spot * steps + i, 0) if by_rows else (i, spot)

    shape = (4 * rows, width) if by_rows else (rows, 4 * width)
    return pl.pallas_call(
        place_kernel,
        grid_spec=pltpu.PrefetchScalarGridSpec(num_scalar_prefetch=1, grid=(4, steps), in_specs=[source(k) for k in range(4)], out_specs=[pl.BlockSpec((tile, width), target)] * count),
        out_shape=[jax.ShapeDtypeStruct(shape, srcs[0].dtype)] * count,
        cost_estimate=pl.CostEstimate(flops=4 * rows * cols * 512, bytes_accessed=16 * rows * cols, transcendentals=0),
        name="place",
    )(base.reshape(1).astype(jnp.int32), *srcs)


def mlp_kernel(chunk, x_ref, oa_ref, ob_ref, oc_ref, od_ref, wo_ref, ga_ref, gb_ref, gc_ref, gd_ref, da_ref, db_ref, dc_ref, dd_ref, gain_ref,
               y_ref, land_in, land_across,
               wo_v, gu_v, down_v, x_v, o_v, h_v, u_v, acc_v, part_v, half_v, stage_v, y_v,
               w_sem, in_sem, stage_sem, in_send, in_recv, ac_send, ac_recv, out_send, out_recv, y_sem):
    rows_all, dim = x_ref.shape
    count = rows_all // chunk
    heads = oa_ref.shape[1]
    ff = da_ref.shape[0]
    part_id = lax.axis_index('part')
    z = lax.axis_index('tpa')
    tpb = lax.axis_index('tpb')
    is_end = (z == 0) | (z == 3)
    is_mid = (z == 1) | (z == 2)

    def device(row):
        return (part_id, row, tpb)

    mesh_ids = pl.DeviceIdType.MESH
    inner = 1 + z // 2
    other = 3 - z
    outer = 3 * (z // 2)
    barrier = pltpu.get_barrier_semaphore()

    @pl.when(is_end)
    def _():
        pl.semaphore_signal(barrier, 1, device_id=device(inner), device_id_type=mesh_ids)
        pl.semaphore_wait(barrier, 1)

    @pl.when(is_mid)
    def _():
        pl.semaphore_signal(barrier, 1, device_id=device(outer), device_id_type=mesh_ids)
        pl.semaphore_signal(barrier, 1, device_id=device(other), device_id_type=mesh_ids)
        pl.semaphore_wait(barrier, 2)

    near = z + 1 - 2 * (z % 2)
    far = (z + 2) % 4
    both = far + 1 - 2 * (far % 2)
    sources = ((oa_ref, z), (ob_ref, near), (oc_ref, far), (od_ref, both))

    def rows_of(k):
        return pl.ds(pl.multiple_of(k * chunk, chunk), chunk)

    def inputs(k):
        slot = k % 2
        copies = [pltpu.make_async_copy(x_ref.at[rows_of(k)], x_v.at[slot], in_sem.at[slot, 4])]
        for n, (ref, spot) in enumerate(sources):
            cols = pl.ds(pl.multiple_of(spot * heads, heads), heads)
            copies.append(pltpu.make_async_copy(ref.at[rows_of(k)], o_v.at[slot, :, cols], in_sem.at[slot, n]))
        return copies

    weights = [pltpu.make_async_copy(wo_ref, wo_v, w_sem.at[8])]
    for n, (g_ref, d_ref) in enumerate(((ga_ref, da_ref), (gb_ref, db_ref), (gc_ref, dc_ref), (gd_ref, dd_ref))):
        weights.append(pltpu.make_async_copy(g_ref, gu_v.at[n], w_sem.at[2 * n]))
        weights.append(pltpu.make_async_copy(d_ref, down_v.at[n], w_sem.at[2 * n + 1]))
    for copy in inputs(0) + weights:
        copy.start()
    for copy in weights:
        copy.wait()

    def send_in(k):
        return pltpu.make_async_remote_copy(src_ref=part_v.at[k % 3], dst_ref=land_in.at[rows_of(k)], send_sem=in_send.at[k], recv_sem=in_recv.at[k], device_id=device(inner), device_id_type=mesh_ids)

    def send_across(k):
        return pltpu.make_async_remote_copy(src_ref=half_v.at[k % 3], dst_ref=land_across.at[rows_of(k)], send_sem=ac_send.at[k], recv_sem=ac_recv.at[k], device_id=device(other), device_id_type=mesh_ids)

    def send_out(k):
        return pltpu.make_async_remote_copy(src_ref=y_v.at[k % 2], dst_ref=y_ref.at[rows_of(k)], send_sem=out_send.at[k], recv_sem=out_recv.at[k], device_id=device(outer), device_id_type=mesh_ids)

    def keep_out(k):
        return pltpu.make_async_copy(y_v.at[k % 2], y_ref.at[rows_of(k)], y_sem.at[k % 2])

    def fetch(ref, k, slot):
        return pltpu.make_async_copy(ref.at[rows_of(k)], stage_v.at[slot], stage_sem.at[slot])

    def step(k, carry):
        @pl.when(k < count)
        def _():
            for copy in inputs(k):
                copy.wait()

            @pl.when(k + 1 < count)
            def _():
                for copy in inputs(k + 1):
                    copy.start()

            @pl.when(is_end & (k >= 3))
            def _():
                send_in(k - 3).wait_send()

            slot = k % 2
            hidden = (x_v[slot].astype(jnp.float32) + jnp.dot(o_v[slot], wo_v[...], preferred_element_type=jnp.float32)).astype(jnp.bfloat16)
            h_v[k % 3] = hidden
            wide = hidden.astype(jnp.float32)
            mean_sq = jnp.mean(wide * wide, axis=1, keepdims=True)
            u_v[...] = (wide * lax.rsqrt(mean_sq + NORM_EPS) * gain_ref[...].astype(jnp.float32)).astype(jnp.bfloat16)
            acc_v[...] = jnp.zeros_like(acc_v)

            def ff_block(r, inner_carry):
                gate_up = jnp.dot(u_v[...], gu_v[r], preferred_element_type=jnp.float32)
                gate = gate_up[:, :ff].astype(jnp.bfloat16).astype(jnp.float32)
                up = gate_up[:, ff:].astype(jnp.bfloat16).astype(jnp.float32)
                mid = (jax.nn.silu(gate) * up).astype(jnp.bfloat16)
                acc_v[...] += jnp.dot(mid, down_v[r], preferred_element_type=jnp.float32)
                return inner_carry

            lax.fori_loop(0, 4, ff_block, 0)
            part_v[k % 3] = acc_v[...].astype(jnp.bfloat16)

            @pl.when(is_end)
            def _():
                send_in(k).start()

        @pl.when(is_mid & (k >= 1) & (k <= count))
        def _():
            j = k - 1
            send_in(j).wait_recv()
            copy = fetch(land_in, j, 0)
            copy.start()

            @pl.when(j >= 3)
            def _():
                send_across(j - 3).wait_send()

            copy.wait()
            half_v[j % 3] = (part_v[j % 3].astype(jnp.float32) + stage_v[0].astype(jnp.float32)).astype(jnp.bfloat16)
            send_across(j).start()

        @pl.when(is_mid & (k >= 2))
        def _():
            j = k - 2
            send_across(j).wait_recv()
            copy = fetch(land_across, j, 1)
            copy.start()

            @pl.when(j >= 2)
            def _():
                send_out(j - 2).wait_send()
                keep_out(j - 2).wait()

            copy.wait()
            total = half_v[j % 3].astype(jnp.float32) + stage_v[1].astype(jnp.float32)
            y_v[j % 2] = (h_v[j % 3].astype(jnp.float32) + total).astype(jnp.bfloat16)
            send_out(j).start()
            keep_out(j).start()

        return carry

    lax.fori_loop(0, count + 2, step, 0)

    @pl.when(is_end)
    def _():
        for k in range(count - 3, count):
            send_in(k).wait_send()

        def arrive(k, carry):
            send_out(k).wait_recv()
            return carry

        lax.fori_loop(0, count, arrive, 0)

    @pl.when(is_mid)
    def _():
        for k in range(count - 3, count):
            send_across(k).wait_send()
        for k in range(count - 2, count):
            send_out(k).wait_send()
            keep_out(k).wait()


def mlp(x_flat, heads, w_o_all, gu, down, gain, chunk):
    rows, dim = x_flat.shape
    count = rows // chunk
    ff = down[0].shape[0]
    anywhere = pl.BlockSpec(memory_space=pl.ANY)
    whole = jax.ShapeDtypeStruct((rows, dim), jnp.bfloat16)
    inner = w_o_all.shape[0]
    dma = pltpu.SemaphoreType.DMA
    out = pl.pallas_call(
        functools.partial(mlp_kernel, chunk),
        in_specs=[anywhere] * 14 + [pl.BlockSpec(memory_space=pltpu.VMEM)],
        out_specs=[anywhere] * 3,
        out_shape=[whole] * 3,
        scratch_shapes=[
            pltpu.VMEM((inner, dim), jnp.bfloat16), pltpu.VMEM((4, dim, 2 * ff), jnp.bfloat16), pltpu.VMEM((4, ff, dim), jnp.bfloat16),
            pltpu.VMEM((2, chunk, dim), jnp.bfloat16), pltpu.VMEM((2, chunk, inner), jnp.bfloat16), pltpu.VMEM((3, chunk, dim), jnp.bfloat16),
            pltpu.VMEM((chunk, dim), jnp.bfloat16), pltpu.VMEM((chunk, dim), jnp.float32), pltpu.VMEM((3, chunk, dim), jnp.bfloat16),
            pltpu.VMEM((3, chunk, dim), jnp.bfloat16), pltpu.VMEM((2, chunk, dim), jnp.bfloat16), pltpu.VMEM((2, chunk, dim), jnp.bfloat16),
            dma((9,)), dma((2, 5)), dma((2,)), dma((count,)), dma((count,)), dma((count,)), dma((count,)), dma((count,)), dma((count,)), dma((2,)),
        ],
        compiler_params=pltpu.CompilerParams(collective_id=1, has_side_effects=True, vmem_limit_bytes=63 * 1024 * 1024),
        cost_estimate=pl.CostEstimate(flops=2 * rows * dim * (inner + 12 * ff), bytes_accessed=8 * rows * dim, transcendentals=4 * rows * ff),
        name="mlp",
    )(x_flat, *heads, w_o_all, *gu, *down, gain.reshape(1, dim))
    return out[0]


def gather_blocks(block):
    chip = lax.ppermute(block, 'tpb', OTHER_CHIP)
    core = lax.ppermute(block, 'tpb', OTHER_CORE)
    return block, core, chip, lax.ppermute(chip, 'tpb', OTHER_CORE)


def dot(a, b):
    return jnp.dot(a, b, preferred_element_type=jnp.float32)


def local_step(x_loc, len_loc, k_buf, v_buf, w_qkv, w_o, w_gate_up, w_down, g_attn, g_mlp):
    batch, seq, model_dim = x_loc.shape
    tpa = lax.axis_index('tpa')
    tpb = lax.axis_index('tpb')
    ff_block = w_down.shape[0]
    x_flat = x_loc.reshape(batch * seq, model_dim)

    qkv_own = lax.all_gather(w_qkv, 'tpb', axis=1, tiled=True)
    far = lax.ppermute(w_qkv, 'tpa', FAR_ROW)
    normed, far = lax.optimization_barrier((rms_norm(x_flat, g_attn), far))
    qkv_far = lax.all_gather(far, 'tpb', axis=1, tiled=True)
    w_o_all = lax.all_gather(w_o, ('tpa', 'tpb'), axis=0, tiled=True)
    w_gate_up, w_down, _ = lax.optimization_barrier((w_gate_up, w_down, qkv_own))
    gu = gather_blocks(w_gate_up)
    down = gather_blocks(w_down)
    w_gate, w_up = place(gu, tpb, 2, False)
    w_down_gen, = place(down, tpb, 1, True)

    cos_tab, sin_tab = rope_tables(seq, HEAD)
    cos_wide = jnp.tile(cos_tab, (1, 4))
    sin_wide = jnp.tile(jnp.concatenate([-sin_tab, sin_tab], axis=1), (1, 2))
    positions = jnp.arange(seq)
    at_mask = (jnp.arange(LANES) == HEAD)[None, None, :] & (positions[None, :, None] >= len_loc[:, None, None])
    aug = jnp.where(at_mask, MASK_VALUE, 0.0).astype(jnp.bfloat16)

    aug = aug.reshape(batch * seq, LANES)
    act_own = dot(normed, qkv_own).astype(jnp.bfloat16)
    act_far = dot(normed, qkv_far).astype(jnp.bfloat16)
    heads_own = attention(act_own, cos_wide, sin_wide, aug, batch)
    near_own = lax.ppermute(heads_own, 'tpa', NEAR_ROW)
    heads_far = attention(act_far, cos_wide, sin_wide, aug, batch)
    near_far = lax.ppermute(heads_far, 'tpa', NEAR_ROW)
    layer_out = mlp(x_flat, (heads_own, near_own, heads_far, near_far), w_o_all, gu, down, g_mlp, min(256, seq // 8)).reshape(batch, seq, model_dim)

    kv_local = k_buf.shape[2]
    width = act_own.shape[1] // kv_local
    q_width = width - 2 * HEAD

    def columns(array, begin, size):
        return [array[..., g * width + begin:g * width + begin + size] for g in range(kv_local)]

    act_seq = act_own.reshape(batch, seq, -1)
    k_new = jnp.stack(columns(act_seq, q_width, HEAD), axis=2)
    values = jnp.stack(columns(act_seq, q_width + HEAD, HEAD), axis=2)
    k_rot = apply_rope(k_new.astype(jnp.float32), cos_tab[:, None, :], sin_tab[:, None, :]).astype(jnp.bfloat16)
    valid = (positions[None, :] < len_loc[:, None])[:, :, None, None]
    k_cache = jnp.where(valid, k_rot, k_buf)
    v_cache = jnp.where(valid, values, v_buf)

    w_query = jnp.concatenate(columns(qkv_own, 0, q_width), axis=1)
    w_key = jnp.concatenate(columns(qkv_own, q_width, HEAD), axis=1)
    w_value = jnp.concatenate(columns(qkv_own, q_width + HEAD, HEAD), axis=1)
    o_rows = w_o_all.shape[0] // 4
    w_o_gen = lax.dynamic_slice(w_o_all, (tpa * o_rows, 0), (o_rows, w_o_all.shape[1]))
    return (layer_out, k_cache, v_cache, w_query, w_key, w_value, w_o_gen, w_gate, w_up, w_down_gen)


def solution(mesh):
    batch_spec = P(('part', 'tpb'), None, None)
    len_spec = P(('part', 'tpb'))
    cache_spec = P(('part', 'tpb'), None, 'tpa', None)
    train_cols = P('part', ('tpa', 'tpb'))
    train_rows = P(('part', 'tpa', 'tpb'), None)
    gain_spec = P('part')
    gen_cols = P('part', 'tpa')
    gen_rows = P(('part', 'tpa'), None)
    return jax.shard_map(local_step, mesh=mesh, in_specs=(batch_spec, len_spec, cache_spec, cache_spec, train_cols, train_rows, train_cols, train_rows, gain_spec, gain_spec), out_specs=(batch_spec, cache_spec, cache_spec, gen_cols, gen_cols, gen_cols, gen_rows, gen_cols, gen_cols, gen_rows), check_vma=False)
```

```python
import functools
import math
import jax
import jax.numpy as jnp
from jax import lax
from jax.sharding import PartitionSpec as P
from jax.experimental import pallas as pl
from jax.experimental.pallas import tpu as pltpu

ROPE_BASE = 500000.0
ROPE_FACTOR = 8.0
LOW_FREQ = 1.0
HIGH_FREQ = 4.0
ORIG_CONTEXT = 8192.0
NORM_EPS = 1e-5
MASK_VALUE = -1e30
HEAD = 64
LANES = 128

FAR_ROW = [(0, 2), (2, 0), (1, 3), (3, 1)]
NEAR_ROW = [(0, 1), (1, 0), (2, 3), (3, 2)]
OTHER_CHIP = [(0, 2), (2, 0), (1, 3), (3, 1)]
OTHER_CORE = [(0, 1), (1, 0), (2, 3), (3, 2)]


def rms_norm(x_in, gain_vec):
    x_wide = x_in.astype(jnp.float32)
    mean_sq = jnp.mean(x_wide * x_wide, axis=-1, keepdims=True)
    return (x_wide * lax.rsqrt(mean_sq + NORM_EPS) * gain_vec.astype(jnp.float32)).astype(jnp.bfloat16)


def rope_tables(seq_len, head_dim):
    exponent = jnp.arange(head_dim // 2, dtype=jnp.float32) * (2.0 / head_dim)
    inv_freq = 1.0 / jnp.power(ROPE_BASE, exponent)
    wavelen = 2.0 * math.pi / inv_freq
    smooth = (ORIG_CONTEXT / wavelen - LOW_FREQ) / (HIGH_FREQ - LOW_FREQ)
    blended = (1.0 - smooth) * inv_freq / ROPE_FACTOR + smooth * inv_freq
    rope_freq = jnp.where(wavelen < ORIG_CONTEXT / HIGH_FREQ, inv_freq, jnp.where(wavelen > ORIG_CONTEXT / LOW_FREQ, inv_freq / ROPE_FACTOR, blended))
    angles = jnp.arange(seq_len, dtype=jnp.float32)[:, None] * rope_freq[None, :]
    return jnp.cos(angles), jnp.sin(angles)


def apply_rope(vec_in, cos_tab, sin_tab):
    half_dim = vec_in.shape[-1] // 2
    first_half = vec_in[..., :half_dim]
    second_half = vec_in[..., half_dim:]
    return jnp.concatenate([first_half * cos_tab - second_half * sin_tab, second_half * cos_tab + first_half * sin_tab], axis=-1)


def attn_kernel(tile, q_ref, kv_ref, cos_ref, sin_ref, aug_ref, o_ref, qe_s, qo_s, k_s, ve_s, vo_s):
    seq = q_ref.shape[0]
    lane = lax.broadcasted_iota(jnp.int32, (tile, LANES), 1)
    low = lane < HEAD
    first = lax.rem(lane, HEAD) < HEAD // 2
    ones = jnp.ones((tile, LANES), jnp.float32)
    hot = jnp.where(lane == HEAD, 1.0, 0.0)

    def rope(val, cos, sin):
        rot = jnp.where(first, pltpu.roll(val, LANES - HEAD // 2, 1), pltpu.roll(val, HEAD // 2, 1))
        return val * cos + rot * sin

    for i in range(seq // tile):
        rows = slice(i * tile, (i + 1) * tile)
        cos, sin = cos_ref[rows, :], sin_ref[rows, :]
        q = rope(q_ref[rows, :].astype(jnp.float32), cos, sin).astype(jnp.bfloat16).astype(jnp.float32) * HEAD ** -0.5
        qe_s[rows, :] = jnp.where(low, q, hot).astype(jnp.bfloat16)
        qo_s[rows, :] = jnp.where(low, pltpu.roll(q, HEAD, 1), hot).astype(jnp.bfloat16)
        kv = kv_ref[rows, :].astype(jnp.float32)
        k_s[rows, :] = jnp.where(low, rope(kv, cos, sin), aug_ref[rows, :].astype(jnp.float32)).astype(jnp.bfloat16)
        ve_s[rows, :] = jnp.where(low, pltpu.roll(kv, HEAD, 1), ones).astype(jnp.bfloat16)
        vo_s[rows, :] = jnp.where(low, ones, kv).astype(jnp.bfloat16)
    causal = lax.broadcasted_iota(jnp.int32, (tile, tile), 1) <= lax.broadcasted_iota(jnp.int32, (tile, tile), 0)
    dims = (((1,), (1,)), ((), ()))
    for i in range(seq // tile):
        rows = slice(i * tile, (i + 1) * tile)
        outs = []
        for qs, vs in ((qe_s, ve_s), (qo_s, vo_s)):
            q = qs[rows, :]
            diag = jnp.where(causal, lax.dot_general(q, k_s[rows, :], dims, preferred_element_type=jnp.float32), MASK_VALUE)
            top = jnp.max(diag, axis=1, keepdims=True)
            if i:
                past = lax.dot_general(q, k_s[:i * tile, :], dims, preferred_element_type=jnp.float32)
                top = jnp.maximum(top, jnp.max(past, axis=1, keepdims=True))
            out = jnp.dot(jnp.exp(diag - top).astype(jnp.bfloat16), vs[rows, :], preferred_element_type=jnp.float32)
            if i:
                out = out + jnp.dot(jnp.exp(past - top).astype(jnp.bfloat16), vs[:i * tile, :], preferred_element_type=jnp.float32)
            outs.append(out)
        num = jnp.where(low, outs[0], outs[1])
        den = pltpu.roll(jnp.where(low, outs[1], outs[0]), HEAD, 1)
        o_ref[rows, :] = (num / den).astype(jnp.bfloat16)


def attention(qkv, cos, sin, aug, prompt):
    cols = qkv.shape[1]
    seq = cos.shape[0]
    groups = cols // (3 * LANES)
    tile = min(512, seq)

    def block(index):
        return pl.BlockSpec((seq, LANES), index)

    return pl.pallas_call(
        functools.partial(attn_kernel, tile),
        grid=(groups, 2),
        in_specs=[block(lambda g, p: (prompt, 3 * g + p)), block(lambda g, p: (prompt, 3 * g + 2)), block(lambda g, p: (0, 0)), block(lambda g, p: (0, 0)), block(lambda g, p: (prompt, 0))],
        out_specs=block(lambda g, p: (0, 2 * g + p)),
        out_shape=jax.ShapeDtypeStruct((seq, groups * 2 * LANES), jnp.bfloat16),
        scratch_shapes=[pltpu.VMEM((seq, LANES), jnp.bfloat16)] * 5,
        cost_estimate=pl.CostEstimate(flops=groups * 16 * seq * seq * LANES, bytes_accessed=seq * groups * 2560, transcendentals=groups * 2 * seq * seq),
        name="attention",
    )(qkv, qkv, cos, sin, aug)


def place_kernel(base_ref, *refs):
    outs = refs[4:]
    width = outs[0].shape[1]
    for k in range(4):
        @pl.when(pl.program_id(0) == k)
        def _(k=k):
            for n, out in enumerate(outs):
                out[...] = refs[k][:, n * width:(n + 1) * width]


def place(srcs, base, count, by_rows):
    rows, cols = srcs[0].shape
    width = cols // count
    tile = min(512, rows)
    steps = rows // tile

    def source(k):
        return pl.BlockSpec((tile, cols), lambda r, i, base: (jnp.where(r == k, i, jnp.where(r < k, 0, steps - 1)), 0))

    def target(r, i, base):
        spot = base[0] ^ r
        return (spot * steps + i, 0) if by_rows else (i, spot)

    shape = (4 * rows, width) if by_rows else (rows, 4 * width)
    return pl.pallas_call(
        place_kernel,
        grid_spec=pltpu.PrefetchScalarGridSpec(num_scalar_prefetch=1, grid=(4, steps), in_specs=[source(k) for k in range(4)], out_specs=[pl.BlockSpec((tile, width), target)] * count),
        out_shape=[jax.ShapeDtypeStruct(shape, srcs[0].dtype)] * count,
        cost_estimate=pl.CostEstimate(flops=4 * rows * cols * 512, bytes_accessed=16 * rows * cols, transcendentals=0),
        name="place",
    )(base.reshape(1).astype(jnp.int32), *srcs)


def mlp_kernel(chunk, batch, *refs):
    x_ref, *refs = refs
    heads_refs, refs = refs[:4 * batch], refs[4 * batch:]
    (wo_ref, ga_ref, gb_ref, gc_ref, gd_ref, da_ref, db_ref, dc_ref, dd_ref, gain_ref,
     y_ref, land_in, land_across,
     wo_v, gu_v, down_v, x_v, o_v, h_v, u_v, acc_v, part_v, half_v, stage_v, y_v,
     w_sem, in_sem, stage_sem, in_send, in_recv, ac_send, ac_recv, out_send, out_recv, y_sem, tail_sem) = refs
    rows_all, _ = x_ref.shape
    count = rows_all // chunk
    heads = heads_refs[0].shape[1]
    per_prompt = count // batch
    last = count - 1
    half_rows = chunk // 2
    ff = da_ref.shape[0]
    part_id = lax.axis_index('part')
    z = lax.axis_index('tpa')
    tpb = lax.axis_index('tpb')
    is_end = (z == 0) | (z == 3)
    is_mid = (z == 1) | (z == 2)

    def device(row):
        return (part_id, row, tpb)

    mesh_ids = pl.DeviceIdType.MESH
    inner = 1 + z // 2
    other = 3 - z
    outer = 3 * (z // 2)
    barrier = pltpu.get_barrier_semaphore()

    @pl.when(is_end)
    def _():
        pl.semaphore_signal(barrier, 1, device_id=device(inner), device_id_type=mesh_ids)
        pl.semaphore_wait(barrier, 1)

    @pl.when(is_mid)
    def _():
        pl.semaphore_signal(barrier, 1, device_id=device(outer), device_id_type=mesh_ids)
        pl.semaphore_signal(barrier, 1, device_id=device(other), device_id_type=mesh_ids)
        pl.semaphore_wait(barrier, 2)

    near = z + 1 - 2 * (z % 2)
    far = (z + 2) % 4
    both = far + 1 - 2 * (far % 2)
    spots = (z, near, far, both)

    def rows_of(k):
        return pl.ds(pl.multiple_of(k * chunk, chunk), chunk)

    def input_copies(k, prompt):
        slot = k % 2
        copies = [pltpu.make_async_copy(x_ref.at[rows_of(k)], x_v.at[slot], in_sem.at[slot, 4])]
        for n, spot in enumerate(spots):
            cols = pl.ds(pl.multiple_of(spot * heads, heads), heads)
            copies.append(pltpu.make_async_copy(heads_refs[4 * prompt + n].at[rows_of(k % per_prompt)], o_v.at[slot, :, cols], in_sem.at[slot, n]))
        return copies

    def start_inputs(k):
        for prompt in range(batch):
            @pl.when(k // per_prompt == prompt)
            def _(prompt=prompt):
                for copy in input_copies(k, prompt):
                    copy.start()

    weights = [pltpu.make_async_copy(wo_ref, wo_v, w_sem.at[8])]
    for n, (g_ref, d_ref) in enumerate(((ga_ref, da_ref), (gb_ref, db_ref), (gc_ref, dc_ref), (gd_ref, dd_ref))):
        weights.append(pltpu.make_async_copy(g_ref, gu_v.at[n], w_sem.at[2 * n]))
        weights.append(pltpu.make_async_copy(d_ref, down_v.at[n], w_sem.at[2 * n + 1]))
    for copy in input_copies(0, 0) + weights:
        copy.start()

    def send_in(k):
        return pltpu.make_async_remote_copy(src_ref=part_v.at[k % 3], dst_ref=land_in.at[rows_of(k)], send_sem=in_send.at[k], recv_sem=in_recv.at[k], device_id=device(inner), device_id_type=mesh_ids)

    def send_across(k):
        return pltpu.make_async_remote_copy(src_ref=half_v.at[k % 3], dst_ref=land_across.at[rows_of(k)], send_sem=ac_send.at[k], recv_sem=ac_recv.at[k], device_id=device(other), device_id_type=mesh_ids)

    def send_out(k):
        return pltpu.make_async_remote_copy(src_ref=y_v.at[k % 2], dst_ref=y_ref.at[rows_of(k)], send_sem=out_send.at[k], recv_sem=out_recv.at[k], device_id=device(outer), device_id_type=mesh_ids)

    def keep_out(k):
        return pltpu.make_async_copy(y_v.at[k % 2], y_ref.at[rows_of(k)], y_sem.at[k % 2])

    def tail(ref, n):
        return ref.at[pl.ds(last * chunk + n * half_rows, half_rows)]

    def tail_copy(src, dst, row, which, n):
        return pltpu.make_async_remote_copy(src_ref=src.at[:, pl.ds(n * half_rows, half_rows)].at[0], dst_ref=tail(dst, n), send_sem=tail_sem.at[which, n], recv_sem=tail_sem.at[which + 1, n], device_id=device(row), device_id_type=mesh_ids)

    def tail_in(n):
        return tail_copy(part_v.at[pl.ds(last % 3, 1)], land_in, inner, 0, n)

    def tail_across(n):
        return tail_copy(half_v.at[pl.ds(last % 3, 1)], land_across, other, 2, n)

    def tail_out(n):
        return tail_copy(y_v.at[pl.ds(last % 2, 1)], y_ref, outer, 4, n)

    def tail_keep(n):
        return pltpu.make_async_copy(y_v.at[last % 2, pl.ds(n * half_rows, half_rows)], tail(y_ref, n), tail_sem.at[6, n])

    def tail_fetch(ref, slot, n):
        return pltpu.make_async_copy(tail(ref, n), stage_v.at[slot, pl.ds(n * half_rows, half_rows)], tail_sem.at[7, n])

    def fetch(ref, k, slot):
        return pltpu.make_async_copy(ref.at[rows_of(k)], stage_v.at[slot], stage_sem.at[slot])

    def step(k, carry):
        @pl.when(k < count)
        def _():
            for copy in input_copies(k, 0):
                copy.wait()

            @pl.when(k + 1 < count)
            def _():
                start_inputs(k + 1)

            @pl.when(k == 0)
            def _():
                weights[0].wait()

            @pl.when(is_end & (k >= 3))
            def _():
                send_in(k - 3).wait_send()

            slot = k % 2
            hidden = (x_v[slot].astype(jnp.float32) + jnp.dot(o_v[slot], wo_v[...], preferred_element_type=jnp.float32)).astype(jnp.bfloat16)
            h_v[k % 3] = hidden
            wide = hidden.astype(jnp.float32)
            mean_sq = jnp.mean(wide * wide, axis=1, keepdims=True)
            u_v[...] = (wide * lax.rsqrt(mean_sq + NORM_EPS) * gain_ref[...].astype(jnp.float32)).astype(jnp.bfloat16)
            acc_v[...] = jnp.zeros_like(acc_v)

            def ff_block(r, inner_carry):
                @pl.when(k == 0)
                def _():
                    pltpu.make_async_copy(ga_ref, gu_v.at[r], w_sem.at[2 * r]).wait()
                    pltpu.make_async_copy(da_ref, down_v.at[r], w_sem.at[2 * r + 1]).wait()

                gate_up = jnp.dot(u_v[...], gu_v[r], preferred_element_type=jnp.float32)
                gate = gate_up[:, :ff].astype(jnp.bfloat16).astype(jnp.float32)
                up = gate_up[:, ff:].astype(jnp.bfloat16).astype(jnp.float32)
                mid = (jax.nn.silu(gate) * up).astype(jnp.bfloat16)
                acc_v[...] += jnp.dot(mid, down_v[r], preferred_element_type=jnp.float32)
                return inner_carry

            lax.fori_loop(0, 4, ff_block, 0)
            part_v[k % 3] = acc_v[...].astype(jnp.bfloat16)

            @pl.when(is_end & (k < last))
            def _():
                send_in(k).start()

            @pl.when(is_end & (k == last))
            def _():
                for n in range(2):
                    tail_in(n).start()

        @pl.when(is_mid & (k >= 1) & (k < count))
        def _():
            j = k - 1
            send_in(j).wait_recv()
            copy = fetch(land_in, j, 0)
            copy.start()

            @pl.when(j >= 3)
            def _():
                send_across(j - 3).wait_send()

            copy.wait()
            half_v[j % 3] = (part_v[j % 3].astype(jnp.float32) + stage_v[0].astype(jnp.float32)).astype(jnp.bfloat16)
            send_across(j).start()

        @pl.when(is_mid & (k == count))
        def _():
            send_across(last - 3).wait_send()
            for n in range(2):
                tail_in(n).wait_recv()
                copy = tail_fetch(land_in, 0, n)
                copy.start()
                copy.wait()
                rows = slice(n * half_rows, (n + 1) * half_rows)
                half_v[last % 3, rows, :] = (part_v[last % 3, rows, :].astype(jnp.float32) + stage_v[0, rows, :].astype(jnp.float32)).astype(jnp.bfloat16)
                tail_across(n).start()

        @pl.when(is_mid & (k >= 2) & (k <= count))
        def _():
            j = k - 2
            send_across(j).wait_recv()
            copy = fetch(land_across, j, 1)
            copy.start()

            @pl.when(j >= 2)
            def _():
                send_out(j - 2).wait_send()
                keep_out(j - 2).wait()

            copy.wait()
            total = half_v[j % 3].astype(jnp.float32) + stage_v[1].astype(jnp.float32)
            y_v[j % 2] = (h_v[j % 3].astype(jnp.float32) + total).astype(jnp.bfloat16)
            send_out(j).start()
            keep_out(j).start()

        @pl.when(is_mid & (k > count))
        def _():
            send_out(last - 2).wait_send()
            keep_out(last - 2).wait()
            for n in range(2):
                tail_across(n).wait_recv()
                copy = tail_fetch(land_across, 1, n)
                copy.start()
                copy.wait()
                rows = slice(n * half_rows, (n + 1) * half_rows)
                total = half_v[last % 3, rows, :].astype(jnp.float32) + stage_v[1, rows, :].astype(jnp.float32)
                y_v[last % 2, rows, :] = (h_v[last % 3, rows, :].astype(jnp.float32) + total).astype(jnp.bfloat16)
                tail_out(n).start()
                tail_keep(n).start()

        return carry

    lax.fori_loop(0, count + 2, step, 0)

    @pl.when(is_end)
    def _():
        for k in range(count - 3, last):
            send_in(k).wait_send()

        def arrive(k, carry):
            send_out(k).wait_recv()
            return carry

        lax.fori_loop(0, last, arrive, 0)
        for n in range(2):
            tail_in(n).wait_send()
            tail_out(n).wait_recv()

    @pl.when(is_mid)
    def _():
        for k in range(count - 3, last):
            send_across(k).wait_send()
        send_out(last - 1).wait_send()
        keep_out(last - 1).wait()
        for n in range(2):
            tail_across(n).wait_send()
            tail_out(n).wait_send()
            tail_keep(n).wait()


def mlp(x_flat, heads, w_o_all, gu, down, gain, chunk, batch):
    rows, dim = x_flat.shape
    count = rows // chunk
    ff = down[0].shape[0]
    anywhere = pl.BlockSpec(memory_space=pl.ANY)
    whole = jax.ShapeDtypeStruct((rows, dim), jnp.bfloat16)
    inner = w_o_all.shape[0]
    dma = pltpu.SemaphoreType.DMA
    out = pl.pallas_call(
        functools.partial(mlp_kernel, chunk, batch),
        in_specs=[anywhere] * (10 + 4 * batch) + [pl.BlockSpec(memory_space=pltpu.VMEM)],
        out_specs=[anywhere] * 3,
        out_shape=[whole] * 3,
        scratch_shapes=[
            pltpu.VMEM((inner, dim), jnp.bfloat16), pltpu.VMEM((4, dim, 2 * ff), jnp.bfloat16), pltpu.VMEM((4, ff, dim), jnp.bfloat16),
            pltpu.VMEM((2, chunk, dim), jnp.bfloat16), pltpu.VMEM((2, chunk, inner), jnp.bfloat16), pltpu.VMEM((3, chunk, dim), jnp.bfloat16),
            pltpu.VMEM((chunk, dim), jnp.bfloat16), pltpu.VMEM((chunk, dim), jnp.float32), pltpu.VMEM((3, chunk, dim), jnp.bfloat16),
            pltpu.VMEM((3, chunk, dim), jnp.bfloat16), pltpu.VMEM((2, chunk, dim), jnp.bfloat16), pltpu.VMEM((2, chunk, dim), jnp.bfloat16),
            dma((9,)), dma((2, 5)), dma((2,)), dma((count,)), dma((count,)), dma((count,)), dma((count,)), dma((count,)), dma((count,)), dma((2,)), dma((8, 2)),
        ],
        compiler_params=pltpu.CompilerParams(collective_id=1, has_side_effects=True, vmem_limit_bytes=63 * 1024 * 1024),
        cost_estimate=pl.CostEstimate(flops=2 * rows * dim * (inner + 12 * ff), bytes_accessed=8 * rows * dim, transcendentals=4 * rows * ff),
        name="mlp",
    )(x_flat, *heads, w_o_all, *gu, *down, gain.reshape(1, dim))
    return out[0]


def with_other_core(block, chip):
    return block, lax.ppermute(block, 'tpb', OTHER_CORE), chip, lax.ppermute(chip, 'tpb', OTHER_CORE)


def dot(a, b):
    return jnp.dot(a, b, preferred_element_type=jnp.float32)


def layer(x_loc, len_loc, k_buf, v_buf, w_qkv, w_o, w_gate_up, w_down, g_attn, g_mlp):
    batch, seq, model_dim = x_loc.shape
    tpa = lax.axis_index('tpa')
    tpb = lax.axis_index('tpb')
    x_flat = x_loc.reshape(batch * seq, model_dim)

    qkv_own = lax.all_gather(w_qkv, 'tpb', axis=1, tiled=True)
    far = lax.ppermute(w_qkv, 'tpa', FAR_ROW)
    normed = rms_norm(x_flat, g_attn)
    act_own = dot(normed, qkv_own).astype(jnp.bfloat16)
    act_own, far = lax.optimization_barrier((act_own, far))
    qkv_far = lax.all_gather(far, 'tpb', axis=1, tiled=True)
    w_o_all = lax.all_gather(w_o, ('tpa', 'tpb'), axis=0, tiled=True)
    w_gate_up, w_down, _ = lax.optimization_barrier((w_gate_up, w_down, qkv_own))
    cos_tab, sin_tab = rope_tables(seq, HEAD)
    cos_wide = jnp.tile(cos_tab, (1, 4))
    sin_wide = jnp.tile(jnp.concatenate([-sin_tab, sin_tab], axis=1), (1, 2))
    positions = jnp.arange(seq)
    at_mask = (jnp.arange(LANES) == HEAD)[None, None, :] & (positions[None, :, None] >= len_loc[:, None, None])
    aug = jnp.where(at_mask, MASK_VALUE, 0.0).astype(jnp.bfloat16)

    aug = aug.reshape(batch * seq, LANES)
    act_far = dot(normed, qkv_far).astype(jnp.bfloat16)
    heads_own = [attention(act_own, cos_wide, sin_wide, aug, b) for b in range(batch)]
    heads_far = []
    for b in range(batch):
        heads_far.append(attention(act_far, cos_wide, sin_wide, aug, b))
    gu_chip = lax.ppermute(w_gate_up, 'tpb', OTHER_CHIP)
    down_chip = lax.ppermute(w_down, 'tpb', OTHER_CHIP)
    near_own = [lax.ppermute(h, 'tpa', NEAR_ROW) for h in heads_own]
    near_far = []
    for b in range(batch):
        near_far.append(lax.ppermute(heads_far[b], 'tpa', NEAR_ROW))
    _, gu_chip = lax.optimization_barrier((heads_far[0], gu_chip))
    _, down_chip = lax.optimization_barrier((heads_far[-1], down_chip))
    gu = with_other_core(w_gate_up, gu_chip)
    down = with_other_core(w_down, down_chip)
    w_gate, w_up = place(gu, tpb, 2, False)
    w_down_gen, = place(down, tpb, 1, True)

    heads = []
    for b in range(batch):
        heads += [heads_own[b], near_own[b], heads_far[b], near_far[b]]
    o_rows = w_o_all.shape[0] // 4
    w_o_gen = lax.dynamic_slice(w_o_all, (tpa * o_rows, 0), (o_rows, w_o_all.shape[1]))
    heads[-1], w_o_gen = lax.optimization_barrier((heads[-1], w_o_gen))
    layer_out = mlp(x_flat, heads, w_o_all, gu, down, g_mlp, min(256, seq // 8), batch).reshape(batch, seq, model_dim)

    kv_local = k_buf.shape[2]
    width = act_own.shape[1] // kv_local
    q_width = width - 2 * HEAD

    def columns(array, begin, size):
        return [array[..., g * width + begin:g * width + begin + size] for g in range(kv_local)]

    act_seq = act_own.reshape(batch, seq, -1)
    k_new = jnp.stack(columns(act_seq, q_width, HEAD), axis=2)
    values = jnp.stack(columns(act_seq, q_width + HEAD, HEAD), axis=2)
    k_rot = apply_rope(k_new.astype(jnp.float32), cos_tab[:, None, :], sin_tab[:, None, :]).astype(jnp.bfloat16)
    valid = (positions[None, :] < len_loc[:, None])[:, :, None, None]
    k_cache = jnp.where(valid, k_rot, k_buf)
    v_cache = jnp.where(valid, values, v_buf)

    w_query = jnp.concatenate(columns(qkv_own, 0, q_width), axis=1)
    w_key = jnp.concatenate(columns(qkv_own, q_width, HEAD), axis=1)
    w_value = jnp.concatenate(columns(qkv_own, q_width + HEAD, HEAD), axis=1)
    return (layer_out, k_cache, v_cache, w_query, w_key, w_value, w_o_gen, w_gate, w_up, w_down_gen)


def solution(mesh):
    batch_spec = P(('part', 'tpb'), None, None)
    len_spec = P(('part', 'tpb'))
    cache_spec = P(('part', 'tpb'), None, 'tpa', None)
    train_cols = P('part', ('tpa', 'tpb'))
    train_rows = P(('part', 'tpa', 'tpb'), None)
    gain_spec = P('part')
    gen_cols = P('part', 'tpa')
    gen_rows = P(('part', 'tpa'), None)
    return jax.shard_map(layer, mesh=mesh, in_specs=(batch_spec, len_spec, cache_spec, cache_spec, train_cols, train_rows, train_cols, train_rows, gain_spec, gain_spec), out_specs=(batch_spec, cache_spec, cache_spec, gen_cols, gen_cols, gen_cols, gen_rows, gen_cols, gen_cols, gen_rows), check_vma=False)
```

```python
import functools
import math
import jax
import jax.numpy as jnp
from jax import lax
from jax.sharding import PartitionSpec as P
from jax.experimental import pallas as pl
from jax.experimental.pallas import tpu as pltpu

ROPE_BASE = 500000.0
ROPE_FACTOR = 8.0
LOW_FREQ = 1.0
HIGH_FREQ = 4.0
ORIG_CONTEXT = 8192.0
NORM_EPS = 1e-5
MASK_VALUE = -1e30
HEAD = 64
LANES = 128

FAR_ROW = [(0, 2), (2, 0), (1, 3), (3, 1)]
NEAR_ROW = [(0, 1), (1, 0), (2, 3), (3, 2)]
OTHER_CHIP = [(0, 2), (2, 0), (1, 3), (3, 1)]
OTHER_CORE = [(0, 1), (1, 0), (2, 3), (3, 2)]


def rms_norm(x_in, gain_vec):
    x_wide = x_in.astype(jnp.float32)
    mean_sq = jnp.mean(x_wide * x_wide, axis=-1, keepdims=True)
    return (x_wide * lax.rsqrt(mean_sq + NORM_EPS) * gain_vec.astype(jnp.float32)).astype(jnp.bfloat16)


def rope_tables(seq_len, head_dim):
    exponent = jnp.arange(head_dim // 2, dtype=jnp.float32) * (2.0 / head_dim)
    inv_freq = 1.0 / jnp.power(ROPE_BASE, exponent)
    wavelen = 2.0 * math.pi / inv_freq
    smooth = (ORIG_CONTEXT / wavelen - LOW_FREQ) / (HIGH_FREQ - LOW_FREQ)
    blended = (1.0 - smooth) * inv_freq / ROPE_FACTOR + smooth * inv_freq
    rope_freq = jnp.where(wavelen < ORIG_CONTEXT / HIGH_FREQ, inv_freq, jnp.where(wavelen > ORIG_CONTEXT / LOW_FREQ, inv_freq / ROPE_FACTOR, blended))
    angles = jnp.arange(seq_len, dtype=jnp.float32)[:, None] * rope_freq[None, :]
    return jnp.cos(angles), jnp.sin(angles)


def apply_rope(vec_in, cos_tab, sin_tab):
    half_dim = vec_in.shape[-1] // 2
    first_half = vec_in[..., :half_dim]
    second_half = vec_in[..., half_dim:]
    return jnp.concatenate([first_half * cos_tab - second_half * sin_tab, second_half * cos_tab + first_half * sin_tab], axis=-1)


def attn_kernel(tile, q_ref, kv_ref, cos_ref, sin_ref, aug_ref, o_ref, qe_s, qo_s, k_s, ve_s, vo_s):
    seq = q_ref.shape[0]
    lane = lax.broadcasted_iota(jnp.int32, (tile, LANES), 1)
    low = lane < HEAD
    first = lax.rem(lane, HEAD) < HEAD // 2
    ones = jnp.ones((tile, LANES), jnp.float32)
    hot = jnp.where(lane == HEAD, 1.0, 0.0)

    def rope(val, cos, sin):
        rot = jnp.where(first, pltpu.roll(val, LANES - HEAD // 2, 1), pltpu.roll(val, HEAD // 2, 1))
        return val * cos + rot * sin

    for i in range(seq // tile):
        rows = slice(i * tile, (i + 1) * tile)
        cos, sin = cos_ref[rows, :], sin_ref[rows, :]
        q = rope(q_ref[rows, :].astype(jnp.float32), cos, sin).astype(jnp.bfloat16).astype(jnp.float32) * HEAD ** -0.5
        qe_s[rows, :] = jnp.where(low, q, hot).astype(jnp.bfloat16)
        qo_s[rows, :] = jnp.where(low, pltpu.roll(q, HEAD, 1), hot).astype(jnp.bfloat16)
        kv = kv_ref[rows, :].astype(jnp.float32)
        k_s[rows, :] = jnp.where(low, rope(kv, cos, sin), aug_ref[rows, :].astype(jnp.float32)).astype(jnp.bfloat16)
        ve_s[rows, :] = jnp.where(low, pltpu.roll(kv, HEAD, 1), ones).astype(jnp.bfloat16)
        vo_s[rows, :] = jnp.where(low, ones, kv).astype(jnp.bfloat16)
    causal = lax.broadcasted_iota(jnp.int32, (tile, tile), 1) <= lax.broadcasted_iota(jnp.int32, (tile, tile), 0)
    dims = (((1,), (1,)), ((), ()))
    for i in range(seq // tile):
        rows = slice(i * tile, (i + 1) * tile)
        outs = []
        for qs, vs in ((qe_s, ve_s), (qo_s, vo_s)):
            q = qs[rows, :]
            diag = jnp.where(causal, lax.dot_general(q, k_s[rows, :], dims, preferred_element_type=jnp.float32), MASK_VALUE)
            top = jnp.max(diag, axis=1, keepdims=True)
            if i:
                past = lax.dot_general(q, k_s[:i * tile, :], dims, preferred_element_type=jnp.float32)
                top = jnp.maximum(top, jnp.max(past, axis=1, keepdims=True))
            out = jnp.dot(jnp.exp(diag - top).astype(jnp.bfloat16), vs[rows, :], preferred_element_type=jnp.float32)
            if i:
                out = out + jnp.dot(jnp.exp(past - top).astype(jnp.bfloat16), vs[:i * tile, :], preferred_element_type=jnp.float32)
            outs.append(out)
        num = jnp.where(low, outs[0], outs[1])
        den = pltpu.roll(jnp.where(low, outs[1], outs[0]), HEAD, 1)
        o_ref[rows, :] = (num / den).astype(jnp.bfloat16)


def attention(qkv, cos, sin, aug, prompt):
    cols = qkv.shape[1]
    seq = cos.shape[0]
    groups = cols // (3 * LANES)
    tile = min(512, seq)

    def block(index):
        return pl.BlockSpec((seq, LANES), index)

    return pl.pallas_call(
        functools.partial(attn_kernel, tile),
        grid=(groups, 2),
        in_specs=[block(lambda g, p: (prompt, 3 * g + p)), block(lambda g, p: (prompt, 3 * g + 2)), block(lambda g, p: (0, 0)), block(lambda g, p: (0, 0)), block(lambda g, p: (prompt, 0))],
        out_specs=block(lambda g, p: (0, 2 * g + p)),
        out_shape=jax.ShapeDtypeStruct((seq, groups * 2 * LANES), jnp.bfloat16),
        scratch_shapes=[pltpu.VMEM((seq, LANES), jnp.bfloat16)] * 5,
        cost_estimate=pl.CostEstimate(flops=groups * 16 * seq * seq * LANES, bytes_accessed=seq * groups * 2560, transcendentals=groups * 2 * seq * seq),
        name="attention",
    )(qkv, qkv, cos, sin, aug)


def place_kernel(base_ref, *refs):
    outs = refs[4:]
    width = outs[0].shape[1]
    for k in range(4):
        @pl.when(pl.program_id(0) == k)
        def _(k=k):
            for n, out in enumerate(outs):
                out[...] = refs[k][:, n * width:(n + 1) * width]


def place(srcs, base, count, by_rows):
    rows, cols = srcs[0].shape
    width = cols // count
    tile = min(512, rows)
    steps = rows // tile

    def source(k):
        return pl.BlockSpec((tile, cols), lambda r, i, base: (jnp.where(r == k, i, jnp.where(r < k, 0, steps - 1)), 0))

    def target(r, i, base):
        spot = base[0] ^ r
        return (spot * steps + i, 0) if by_rows else (i, spot)

    shape = (4 * rows, width) if by_rows else (rows, 4 * width)
    return pl.pallas_call(
        place_kernel,
        grid_spec=pltpu.PrefetchScalarGridSpec(num_scalar_prefetch=1, grid=(4, steps), in_specs=[source(k) for k in range(4)], out_specs=[pl.BlockSpec((tile, width), target)] * count),
        out_shape=[jax.ShapeDtypeStruct(shape, srcs[0].dtype)] * count,
        cost_estimate=pl.CostEstimate(flops=4 * rows * cols * 512, bytes_accessed=16 * rows * cols, transcendentals=0),
        name="place",
    )(base.reshape(1).astype(jnp.int32), *srcs)


def mlp_kernel(chunk, batch, *refs):
    x_ref, *refs = refs
    heads_refs, refs = refs[:4 * batch], refs[4 * batch:]
    (wo_ref, ga_ref, gb_ref, gc_ref, gd_ref, da_ref, db_ref, dc_ref, dd_ref, gain_ref,
     y_ref, land_in, land_across,
     wo_v, gu_v, down_v, x_v, o_v, h_v, u_v, acc_v, part_v, half_v, stage_v, y_v,
     w_sem, in_sem, stage_sem, in_send, in_recv, ac_send, ac_recv, out_send, out_recv, y_sem) = refs
    rows_all, _ = x_ref.shape
    count = rows_all // chunk
    heads = heads_refs[0].shape[1]
    per_prompt = count // batch
    ff = da_ref.shape[0]
    part_id = lax.axis_index('part')
    z = lax.axis_index('tpa')
    tpb = lax.axis_index('tpb')
    is_end = (z == 0) | (z == 3)
    is_mid = (z == 1) | (z == 2)

    def device(row):
        return (part_id, row, tpb)

    mesh_ids = pl.DeviceIdType.MESH
    inner = 1 + z // 2
    other = 3 - z
    outer = 3 * (z // 2)
    barrier = pltpu.get_barrier_semaphore()

    @pl.when(is_end)
    def _():
        pl.semaphore_signal(barrier, 1, device_id=device(inner), device_id_type=mesh_ids)
        pl.semaphore_wait(barrier, 1)

    @pl.when(is_mid)
    def _():
        pl.semaphore_signal(barrier, 1, device_id=device(outer), device_id_type=mesh_ids)
        pl.semaphore_signal(barrier, 1, device_id=device(other), device_id_type=mesh_ids)
        pl.semaphore_wait(barrier, 2)

    near = z + 1 - 2 * (z % 2)
    far = (z + 2) % 4
    both = far + 1 - 2 * (far % 2)
    spots = (z, near, far, both)

    def rows_of(k):
        return pl.ds(pl.multiple_of(k * chunk, chunk), chunk)

    def input_copies(k, prompt):
        slot = k % 2
        copies = [pltpu.make_async_copy(x_ref.at[rows_of(k)], x_v.at[slot], in_sem.at[slot, 4])]
        for n, spot in enumerate(spots):
            cols = pl.ds(pl.multiple_of(spot * heads, heads), heads)
            copies.append(pltpu.make_async_copy(heads_refs[4 * prompt + n].at[rows_of(k % per_prompt)], o_v.at[slot, :, cols], in_sem.at[slot, n]))
        return copies

    def start_inputs(k):
        for prompt in range(batch):
            @pl.when(k // per_prompt == prompt)
            def _(prompt=prompt):
                for copy in input_copies(k, prompt):
                    copy.start()

    o_rows = wo_ref.shape[2]
    weights = []
    for t in range(4):
        for row in range(4):
            weights.append(pltpu.make_async_copy(wo_ref.at[t, row], wo_v.at[pl.ds((4 * row + t) * o_rows, o_rows)], w_sem.at[8 + 4 * t + row]))
    for n, (g_ref, d_ref) in enumerate(((ga_ref, da_ref), (gb_ref, db_ref), (gc_ref, dc_ref), (gd_ref, dd_ref))):
        weights.append(pltpu.make_async_copy(g_ref, gu_v.at[n], w_sem.at[2 * n]))
        weights.append(pltpu.make_async_copy(d_ref, down_v.at[n], w_sem.at[2 * n + 1]))
    for copy in input_copies(0, 0) + weights:
        copy.start()

    def send_in(k):
        return pltpu.make_async_remote_copy(src_ref=part_v.at[k % 3], dst_ref=land_in.at[rows_of(k)], send_sem=in_send.at[k], recv_sem=in_recv.at[k], device_id=device(inner), device_id_type=mesh_ids)

    def send_across(k):
        return pltpu.make_async_remote_copy(src_ref=half_v.at[k % 3], dst_ref=land_across.at[rows_of(k)], send_sem=ac_send.at[k], recv_sem=ac_recv.at[k], device_id=device(other), device_id_type=mesh_ids)

    def send_out(k):
        return pltpu.make_async_remote_copy(src_ref=y_v.at[k % 2], dst_ref=y_ref.at[rows_of(k)], send_sem=out_send.at[k], recv_sem=out_recv.at[k], device_id=device(outer), device_id_type=mesh_ids)

    def keep_out(k):
        return pltpu.make_async_copy(y_v.at[k % 2], y_ref.at[rows_of(k)], y_sem.at[k % 2])

    def fetch(ref, k, slot):
        return pltpu.make_async_copy(ref.at[rows_of(k)], stage_v.at[slot], stage_sem.at[slot])

    def step(k, carry):
        takes_in = is_mid & (k >= 2) & (k < count + 2)
        takes_across = is_mid & (k >= 4)

        @pl.when(takes_in)
        def _():
            send_in(k - 2).wait_recv()
            fetch(land_in, k - 2, 0).start()

        @pl.when(takes_across)
        def _():
            send_across(k - 4).wait_recv()
            fetch(land_across, k - 4, 1).start()

        @pl.when(k < count)
        def _():
            for copy in input_copies(k, 0):
                copy.wait()

            @pl.when(k + 1 < count)
            def _():
                start_inputs(k + 1)

            @pl.when(k == 0)
            def _():
                for copy in weights[:16]:
                    copy.wait()

            @pl.when(is_end & (k >= 3))
            def _():
                send_in(k - 3).wait_send()

            slot = k % 2
            hidden = (x_v[slot].astype(jnp.float32) + jnp.dot(o_v[slot], wo_v[...], preferred_element_type=jnp.float32)).astype(jnp.bfloat16)
            h_v[k % 5] = hidden
            wide = hidden.astype(jnp.float32)
            mean_sq = jnp.mean(wide * wide, axis=1, keepdims=True)
            u_v[...] = (wide * lax.rsqrt(mean_sq + NORM_EPS) * gain_ref[...].astype(jnp.float32)).astype(jnp.bfloat16)
            acc_v[...] = jnp.zeros_like(acc_v)

            def ff_block(r, inner_carry):
                @pl.when(k == 0)
                def _():
                    pltpu.make_async_copy(ga_ref, gu_v.at[r], w_sem.at[2 * r]).wait()
                    pltpu.make_async_copy(da_ref, down_v.at[r], w_sem.at[2 * r + 1]).wait()

                gate_up = jnp.dot(u_v[...], gu_v[r], preferred_element_type=jnp.float32)
                gate = gate_up[:, :ff].astype(jnp.bfloat16).astype(jnp.float32)
                up = gate_up[:, ff:].astype(jnp.bfloat16).astype(jnp.float32)
                mid = (jax.nn.silu(gate) * up).astype(jnp.bfloat16)
                acc_v[...] += jnp.dot(mid, down_v[r], preferred_element_type=jnp.float32)
                return inner_carry

            lax.fori_loop(0, 4, ff_block, 0)
            part_v[k % 3] = acc_v[...].astype(jnp.bfloat16)

            @pl.when(is_end)
            def _():
                send_in(k).start()

        @pl.when(takes_in)
        def _():
            j = k - 2

            @pl.when(j >= 3)
            def _():
                send_across(j - 3).wait_send()

            fetch(land_in, j, 0).wait()
            half_v[j % 3] = (part_v[j % 3].astype(jnp.float32) + stage_v[0].astype(jnp.float32)).astype(jnp.bfloat16)
            send_across(j).start()

        @pl.when(takes_across)
        def _():
            j = k - 4

            @pl.when(j >= 2)
            def _():
                send_out(j - 2).wait_send()
                keep_out(j - 2).wait()

            fetch(land_across, j, 1).wait()
            total = half_v[j % 3].astype(jnp.float32) + stage_v[1].astype(jnp.float32)
            y_v[j % 2] = (h_v[j % 5].astype(jnp.float32) + total).astype(jnp.bfloat16)
            send_out(j).start()
            keep_out(j).start()

        return carry

    lax.fori_loop(0, count + 4, step, 0)

    @pl.when(is_end)
    def _():
        for k in range(count - 3, count):
            send_in(k).wait_send()

        def arrive(k, carry):
            send_out(k).wait_recv()
            return carry

        lax.fori_loop(0, count, arrive, 0)

    @pl.when(is_mid)
    def _():
        for k in range(count - 3, count):
            send_across(k).wait_send()
        for k in range(count - 2, count):
            send_out(k).wait_send()
            keep_out(k).wait()


def mlp(x_flat, heads, w_o_all, gu, down, gain, chunk, batch):
    rows, dim = x_flat.shape
    count = rows // chunk
    ff = down[0].shape[0]
    anywhere = pl.BlockSpec(memory_space=pl.ANY)
    whole = jax.ShapeDtypeStruct((rows, dim), jnp.bfloat16)
    inner = w_o_all.shape[0] * w_o_all.shape[1] * w_o_all.shape[2]
    dma = pltpu.SemaphoreType.DMA
    out = pl.pallas_call(
        functools.partial(mlp_kernel, chunk, batch),
        in_specs=[anywhere] * (10 + 4 * batch) + [pl.BlockSpec(memory_space=pltpu.VMEM)],
        out_specs=[anywhere] * 3,
        out_shape=[whole] * 3,
        scratch_shapes=[
            pltpu.VMEM((inner, dim), jnp.bfloat16), pltpu.VMEM((4, dim, 2 * ff), jnp.bfloat16), pltpu.VMEM((4, ff, dim), jnp.bfloat16),
            pltpu.VMEM((2, chunk, dim), jnp.bfloat16), pltpu.VMEM((2, chunk, inner), jnp.bfloat16), pltpu.VMEM((5, chunk, dim), jnp.bfloat16),
            pltpu.VMEM((chunk, dim), jnp.bfloat16), pltpu.VMEM((chunk, dim), jnp.float32), pltpu.VMEM((3, chunk, dim), jnp.bfloat16),
            pltpu.VMEM((3, chunk, dim), jnp.bfloat16), pltpu.VMEM((2, chunk, dim), jnp.bfloat16), pltpu.VMEM((2, chunk, dim), jnp.bfloat16),
            dma((24,)), dma((2, 5)), dma((2,)), dma((count,)), dma((count,)), dma((count,)), dma((count,)), dma((count,)), dma((count,)), dma((2,)),
        ],
        compiler_params=pltpu.CompilerParams(collective_id=1, has_side_effects=True, vmem_limit_bytes=63 * 1024 * 1024),
        cost_estimate=pl.CostEstimate(flops=2 * rows * dim * (inner + 12 * ff), bytes_accessed=8 * rows * dim, transcendentals=4 * rows * ff),
        name="mlp",
    )(x_flat, *heads, w_o_all, *gu, *down, gain.reshape(1, dim))
    return out[0]


def with_other_core(block, chip):
    return block, lax.ppermute(block, 'tpb', OTHER_CORE), chip, lax.ppermute(chip, 'tpb', OTHER_CORE)


def dot(a, b):
    return jnp.dot(a, b, preferred_element_type=jnp.float32)


def layer(x_loc, len_loc, k_buf, v_buf, w_qkv, w_o, w_gate_up, w_down, g_attn, g_mlp):
    batch, seq, model_dim = x_loc.shape
    tpa = lax.axis_index('tpa')
    tpb = lax.axis_index('tpb')
    x_flat = x_loc.reshape(batch * seq, model_dim)

    qkv_own = lax.all_gather(w_qkv, 'tpb', axis=1, tiled=True)
    far = lax.ppermute(w_qkv, 'tpa', FAR_ROW)
    normed = rms_norm(x_flat, g_attn)
    act_own = dot(normed, qkv_own).astype(jnp.bfloat16)
    act_own, far = lax.optimization_barrier((act_own, far))
    qkv_far = lax.all_gather(far, 'tpb', axis=1, tiled=True)
    w_o_all = lax.all_gather(lax.all_gather(w_o, 'tpa', axis=0), 'tpb', axis=0)
    w_gate_up, w_down, _ = lax.optimization_barrier((w_gate_up, w_down, qkv_own))
    cos_tab, sin_tab = rope_tables(seq, HEAD)
    cos_wide = jnp.tile(cos_tab, (1, 4))
    sin_wide = jnp.tile(jnp.concatenate([-sin_tab, sin_tab], axis=1), (1, 2))
    positions = jnp.arange(seq)
    at_mask = (jnp.arange(LANES) == HEAD)[None, None, :] & (positions[None, :, None] >= len_loc[:, None, None])
    aug = jnp.where(at_mask, MASK_VALUE, 0.0).astype(jnp.bfloat16)

    aug = aug.reshape(batch * seq, LANES)
    act_far = dot(normed, qkv_far).astype(jnp.bfloat16)
    heads_own = [attention(act_own, cos_wide, sin_wide, aug, b) for b in range(batch)]
    heads_far = []
    for b in range(batch):
        heads_far.append(attention(act_far, cos_wide, sin_wide, aug, b))
    gu_chip = lax.ppermute(w_gate_up, 'tpb', OTHER_CHIP)
    down_chip = lax.ppermute(w_down, 'tpb', OTHER_CHIP)
    near_own = [lax.ppermute(h, 'tpa', NEAR_ROW) for h in heads_own]
    near_far = []
    for b in range(batch):
        near_far.append(lax.ppermute(heads_far[b], 'tpa', NEAR_ROW))
    _, gu_chip = lax.optimization_barrier((heads_far[0], gu_chip))
    _, down_chip = lax.optimization_barrier((heads_far[-1], down_chip))
    gu = with_other_core(w_gate_up, gu_chip)
    down = with_other_core(w_down, down_chip)
    w_gate, w_up = place(gu, tpb, 2, False)
    w_down_gen, = place(down, tpb, 1, True)

    heads = []
    for b in range(batch):
        heads += [heads_own[b], near_own[b], heads_far[b], near_far[b]]
    w_o_gen = lax.dynamic_index_in_dim(w_o_all, tpa, 1, keepdims=False).reshape(4 * w_o.shape[0], w_o.shape[1])
    heads[-1], w_o_gen = lax.optimization_barrier((heads[-1], w_o_gen))
    layer_out = mlp(x_flat, heads, w_o_all, gu, down, g_mlp, min(256, seq // 8), batch).reshape(batch, seq, model_dim)

    kv_local = k_buf.shape[2]
    width = act_own.shape[1] // kv_local
    q_width = width - 2 * HEAD

    def columns(array, begin, size):
        return [array[..., g * width + begin:g * width + begin + size] for g in range(kv_local)]

    act_seq = act_own.reshape(batch, seq, -1)
    k_new = jnp.stack(columns(act_seq, q_width, HEAD), axis=2)
    values = jnp.stack(columns(act_seq, q_width + HEAD, HEAD), axis=2)
    k_rot = apply_rope(k_new.astype(jnp.float32), cos_tab[:, None, :], sin_tab[:, None, :]).astype(jnp.bfloat16)
    valid = (positions[None, :] < len_loc[:, None])[:, :, None, None]
    k_cache = jnp.where(valid, k_rot, k_buf)
    v_cache = jnp.where(valid, values, v_buf)

    w_query = jnp.concatenate(columns(qkv_own, 0, q_width), axis=1)
    w_key = jnp.concatenate(columns(qkv_own, q_width, HEAD), axis=1)
    w_value = jnp.concatenate(columns(qkv_own, q_width + HEAD, HEAD), axis=1)
    return (layer_out, k_cache, v_cache, w_query, w_key, w_value, w_o_gen, w_gate, w_up, w_down_gen)


def solution(mesh):
    batch_spec = P(('part', 'tpb'), None, None)
    len_spec = P(('part', 'tpb'))
    cache_spec = P(('part', 'tpb'), None, 'tpa', None)
    train_cols = P('part', ('tpa', 'tpb'))
    train_rows = P(('part', 'tpa', 'tpb'), None)
    gain_spec = P('part')
    gen_cols = P('part', 'tpa')
    gen_rows = P(('part', 'tpa'), None)
    return jax.shard_map(layer, mesh=mesh, in_specs=(batch_spec, len_spec, cache_spec, cache_spec, train_cols, train_rows, train_cols, train_rows, gain_spec, gain_spec), out_specs=(batch_spec, cache_spec, cache_spec, gen_cols, gen_cols, gen_cols, gen_rows, gen_cols, gen_cols, gen_rows), check_vma=False)
```
